1024 devices in a mesh: lat: 16 (over x, z_hi), lon: 64 (over y, z_lo, core).
Axes of the slice: x: 4, y: 8, z: 16 (z_hi: 4, z_lo: 4; z = z_hi * 4 + z_lo), core: 2. Of those that a mesh axis runs over, the one named last changes fastest.
Arguments:
- queries: bfloat16 [8, 128, 256, 640], P(None, 'lat', 'lon'), may hold values from -12 to 12
- key_vectors: bfloat16 [8, 128, 256, 640], P(None, 'lat', 'lon'), may hold values from -12 to 12
- values: bfloat16 [8, 128, 256, 640], P(None, 'lat', 'lon'), may hold values from -6 to 6
- upstream: bfloat16 [8, 128, 256, 640], P(None, 'lat', 'lon'), may hold values from -6 to 6
Outputs:
- attended: bfloat16 [8, 128, 256, 640], P(None, 'lat', 'lon')
- grad_queries: bfloat16 [8, 128, 256, 640], P(None, 'lat', 'lon')
- grad_keys: bfloat16 [8, 128, 256, 640], P(None, 'lat', 'lon')
- grad_values: bfloat16 [8, 128, 256, 640], P(None, 'lat', 'lon')
The draws below stay inside these ranges and needn't reach their ends.
All inputs are finite; a program needn't handle non-finite values.
Results may differ from the reference program's by a relative error of at most 0.0044.
The reference program's roundings to bfloat16 on the way count: a program that leaves them out, or rounds other values in their place, can miss the bound.
Values may be sent and summed in bfloat16 or wider, within the bound.
No kernel may reach another device: no remote copies, remote signals or barrier semaphores. Data moves between devices by JAX's collectives and lax.ppermute only.
A program may use at most 32 MiB of HBM per device.

```python
import jax
import jax.numpy as jnp
from jax import lax

BATCH = 8
HEADS = 10
HEAD_DIM = 64
FEAT = 640
LATS = 128
LONS = 256


def drawn_field(key, salt):
    noise = jax.random.normal(jax.random.fold_in(key, salt), (BATCH, LATS, LONS, HEADS * HEAD_DIM), jnp.float32)
    return jnp.clip(noise, -12.0, 12.0).astype(jnp.bfloat16)


def draw_queries(key, part):
    return drawn_field(key, 11)


def draw_key_vectors(key, part):
    return drawn_field(key, 23)


def shard_levels(key, extent, shards, smallest, largest):
    level = 1.0
    for position, parts in shards:
        draws = jax.random.uniform(jax.random.fold_in(jax.random.fold_in(key, 6), position), (parts,), jnp.float32, smallest / len(shards), largest / len(shards))
        level = level * jnp.repeat(jnp.exp(draws), extent[position] // parts).reshape((-1,) + (1,) * (len(extent) - 1 - position))
    return level


def normal_values(key, shape, scale, limit, cuts=(), held_as=jnp.bfloat16):
    gain = shard_levels(key, shape, cuts, -0.22, 0.18) if cuts else 1.0
    entries = jax.random.normal(key, shape, jnp.float32) * scale * gain
    return jnp.minimum(jnp.maximum(entries, -limit), limit).astype(held_as)


def setup_inputs(seed: int = 0) -> dict:
    streams_of = jax.random.split(jax.random.key(seed), 5)
    queries = draw_queries(jax.random.fold_in(streams_of[4], 71), 0)
    key_vectors = draw_key_vectors(jax.random.fold_in(streams_of[4], 71), 0)
    values = normal_values(streams_of[2], (BATCH, LATS, LONS, FEAT), 1.0, 6.0, ((1, 16), (2, 64)))
    upstream = normal_values(streams_of[3], (BATCH, LATS, LONS, FEAT), 1.0, 6.0, ((1, 16), (2, 64)))
    return dict(queries=queries, key_vectors=key_vectors, values=values, upstream=upstream)


def axial_lines(queries, key_vectors, values, upstream):
    count = queries.shape[0]
    length = queries.shape[1]
    heads = queries.shape[2] // HEAD_DIM
    query_heads = queries.astype(jnp.float32).reshape(count, length, heads, HEAD_DIM)
    key_heads = key_vectors.astype(jnp.float32).reshape(count, length, heads, HEAD_DIM)
    value_heads = values.astype(jnp.float32).reshape(count, length, heads, HEAD_DIM)
    grad_heads = upstream.astype(jnp.float32).reshape(count, length, heads, HEAD_DIM)
    score_scale = HEAD_DIM ** -0.5
    scores = jnp.einsum("nqhd,nkhd->nhqk", query_heads, key_heads) * score_scale
    probs = jax.nn.softmax(scores, axis=-1)
    rounded = lax.optimization_barrier(probs.astype(jnp.bfloat16)).astype(jnp.float32)
    output = jnp.einsum("nhqk,nkhd->nqhd", rounded, value_heads)
    grad_probs = jnp.einsum("nqhd,nkhd->nhqk", grad_heads, value_heads)
    row_delta = jnp.sum(probs * grad_probs, axis=-1, keepdims=True)
    grad_scores = probs * (grad_probs - row_delta)
    grad_scores = lax.optimization_barrier(grad_scores.astype(jnp.bfloat16)).astype(jnp.float32)
    grad_value_heads = jnp.einsum("nhqk,nqhd->nkhd", rounded, grad_heads)
    grad_query_heads = jnp.einsum("nhqk,nkhd->nqhd", grad_scores, key_heads) * score_scale
    grad_key_heads = jnp.einsum("nhqk,nqhd->nkhd", grad_scores, query_heads) * score_scale
    results = (output, grad_query_heads, grad_key_heads, grad_value_heads)
    return tuple(item.reshape(count, length, heads * HEAD_DIM).astype(jnp.bfloat16) for item in results)


def one_sample(items):
    queries, key_vectors, values, upstream = items
    along_lon = axial_lines(queries, key_vectors, values, upstream)
    turned = tuple(item.transpose(1, 0, 2) for item in (queries, key_vectors, values, upstream))
    along_lat = tuple(item.transpose(1, 0, 2) for item in axial_lines(*turned))
    return tuple((first.astype(jnp.float32) + second.astype(jnp.float32)).astype(jnp.bfloat16) for first, second in zip(along_lat, along_lon))


def reference(queries, key_vectors, values, upstream):
    attended, grad_queries, grad_keys, grad_values = lax.map(one_sample, (queries, key_vectors, values, upstream))
    return (attended, grad_queries, grad_keys, grad_values)
```

```python
import jax
import jax.numpy as jnp
from jax import lax
from jax.experimental import pallas as pl
from jax.sharding import PartitionSpec as P


HEAD_DIM = 64
HEAD_PAIR = 2 * HEAD_DIM
FACTOR = 4


def attention_kernel(*refs):
    x_refs, o_refs = refs[: len(refs) // 2], refs[len(refs) // 2 :]
    sources, tensors, _, rows, lanes = x_refs[0].shape
    part = sources * rows
    length = part * len(x_refs)
    scale = HEAD_DIM ** (-0.5)

    def whole(t):
        parts = [r[:, t, 0].astype(jnp.float32).reshape(part, lanes) for r in x_refs]
        return jnp.concatenate(parts, axis=0).astype(jnp.bfloat16)

    q, k, v, g = (whole(t) for t in range(tensors))
    lane = lax.broadcasted_iota(jnp.int32, (length, lanes), 1)
    nt, nn, tn = ((((1,), (1,)), ((), ())), (((1,), (0,)), ((), ())), (((0,), (0,)), ((), ())))
    dot = lambda a, b, dims: lax.dot_general(a, b, dims, preferred_element_type=jnp.float32)
    totals = None
    for h in range(lanes // HEAD_DIM):
        mine = lane // HEAD_DIM == h
        qh, kh, vh, gh = (jnp.where(mine, t, jnp.zeros_like(t)) for t in (q, k, v, g))
        scores = dot(qh, kh, nt) * scale
        exps = jnp.exp(scores - jnp.max(scores, axis=-1, keepdims=True))
        probs = exps / jnp.sum(exps, axis=-1, keepdims=True)
        rounded = probs.astype(jnp.bfloat16)
        grad_probs = dot(gh, vh, nt)
        row_delta = jnp.sum(probs * grad_probs, axis=-1, keepdims=True)
        grad_scores = (probs * (grad_probs - row_delta)).astype(jnp.bfloat16)
        parts = (
            dot(rounded, vh, nn),
            dot(grad_scores, kh, nn) * scale,
            dot(grad_scores, qh, tn) * scale,
            dot(rounded, gh, tn),
        )
        totals = parts if totals is None else tuple(a + b for a, b in zip(totals, parts))
    for t in range(tensors):
        for i, r in enumerate(o_refs):
            piece = totals[t][i * part : (i + 1) * part].reshape(sources, rows, lanes)
            r[:, t, 0] = piece.astype(jnp.bfloat16)


def attention(pieces):
    sources, tensors, items, rows, feats = pieces[0].shape
    spec = pl.BlockSpec((sources, tensors, 1, rows, HEAD_PAIR), lambda i, p: (0, 0, i, 0, p))
    return pl.pallas_call(
        attention_kernel,
        grid=(items, feats // HEAD_PAIR),
        in_specs=[spec] * len(pieces),
        out_specs=[spec] * len(pieces),
        out_shape=[jax.ShapeDtypeStruct(p.shape, p.dtype) for p in pieces],
    )(*pieces)


def shift(piece, far, by):
    if by % FACTOR == 0:
        return piece
    place = lambda x, z: x * FACTOR + z
    pairs = []
    for x in range(FACTOR):
        for z in range(FACTOR):
            to = place(x, (z + by) % FACTOR) if far else place((x + by) % FACTOR, z)
            pairs.append((place(x, z), to))
    return lax.ppermute(piece, "lat", pairs)


CHUNKS = 2


def on_device(*inputs):
    batch, rows, cols, feats = inputs[0].shape
    tensors = len(inputs)
    lon = lax.axis_size("lon")
    lat = lax.axis_size("lat")
    lon_items = batch * rows // lon
    lat_items = batch * cols // lat
    me = lax.axis_index("lat")
    near, far = me // FACTOR, me % FACTOR
    swap_lon = lambda t: lax.all_to_all(t, "lon", split_axis=0, concat_axis=0, tiled=True)
    pick = lambda t, i: lax.dynamic_index_in_dim(t, i % FACTOR, 0, keepdims=False)
    part = lat_items // CHUNKS

    lon_got = swap_lon(jnp.stack([t.reshape(lon, lon_items, cols, feats) for t in inputs], axis=1))
    send = jnp.stack([t.transpose(0, 2, 1, 3).reshape(lat, lat_items, rows, feats) for t in inputs], axis=1)
    send = send.reshape((FACTOR, FACTOR) + send.shape[1:])
    far_in = []
    for c in range(CHUNKS):
        mine = send[:, :, :, c * part : (c + 1) * part]
        far_in.append([shift(pick(mine, far + k), True, k) for k in range(FACTOR)])
    (lon_done,) = attention([lon_got])
    lon_back = swap_lon(lon_done)
    home = []
    for c in range(CHUNKS):
        turned = jnp.stack(far_in[c], axis=1)
        got = [shift(pick(turned, near + m), False, m) for m in range(FACTOR)]
        done = attention(got)
        back = [shift(done[m], False, -m) for m in range(FACTOR)]
        home.append([shift(jnp.stack([b[k] for b in back], axis=0), True, -k) for k in range(FACTOR)])
    lat_back = [jnp.roll(jnp.roll(jnp.stack(h, axis=0), far, axis=0), near, axis=1) for h in home]
    lat_back = jnp.concatenate(lat_back, axis=3)
    lat_back = lat_back.reshape((lat,) + lat_back.shape[2:])
    results = []
    for i in range(tensors):
        a = lon_back[:, i].reshape(batch, rows, cols, feats)
        b = lat_back[:, i].reshape(batch, cols, rows, feats).transpose(0, 2, 1, 3)
        results.append((a.astype(jnp.float32) + b.astype(jnp.float32)).astype(jnp.bfloat16))
    return tuple(results)


def solution(mesh):
    spec = P(None, "lat", "lon", None)
    return jax.shard_map(on_device, mesh=mesh, in_specs=(spec,) * 4, out_specs=(spec,) * 4, check_vma=False)
```

```python
import jax
import jax.numpy as jnp
from jax import lax
from jax.experimental import pallas as pl
from jax.experimental.pallas import tpu as pltpu
from jax.sharding import PartitionSpec as P


HEAD_DIM = 64
HEAD_PAIR = 2 * HEAD_DIM
FACTOR = 4
CHUNKS = 2


def attend(x_refs, o_refs, item, lanes):
    sources, tensors, _, rows, _ = x_refs[0].shape
    part = sources * rows
    length = part * len(x_refs)
    scale = HEAD_DIM ** (-0.5)
    full_tiles = rows % 8 == 0

    def whole(t):
        if full_tiles:
            return jnp.concatenate([r[:, t, item, :, lanes].reshape(part, HEAD_PAIR) for r in x_refs], axis=0)
        parts = [r[:, t, item, :, lanes].astype(jnp.float32).reshape(part, HEAD_PAIR) for r in x_refs]
        return jnp.concatenate(parts, axis=0).astype(jnp.bfloat16)

    q, k, v, g = (whole(t) for t in range(tensors))
    lane = lax.broadcasted_iota(jnp.int32, (length, HEAD_PAIR), 1)
    nt, nn, tn = ((((1,), (1,)), ((), ())), (((1,), (0,)), ((), ())), (((0,), (0,)), ((), ())))
    dot = lambda a, b, dims: lax.dot_general(a, b, dims, preferred_element_type=jnp.float32)
    totals = None
    for h in range(HEAD_PAIR // HEAD_DIM):
        mine = lane // HEAD_DIM == h
        qh, kh, vh, gh = (jnp.where(mine, t, jnp.zeros_like(t)) for t in (q, k, v, g))
        scores = dot(qh, k, nt) * scale
        exps = jnp.exp(scores - jnp.max(scores, axis=-1, keepdims=True))
        probs = exps * (1.0 / jnp.sum(exps, axis=-1, keepdims=True))
        rounded = probs.astype(jnp.bfloat16)
        grad_probs = dot(gh, v, nt)
        row_delta = jnp.sum(probs * grad_probs, axis=-1, keepdims=True)
        grad_scores = (probs * (grad_probs - row_delta)).astype(jnp.bfloat16)
        parts = (dot(rounded, vh, nn), dot(grad_scores, kh, nn), dot(grad_scores, qh, tn), dot(rounded, gh, tn))
        totals = parts if totals is None else tuple(a + b for a, b in zip(totals, parts))
    totals = (totals[0], totals[1] * scale, totals[2] * scale, totals[3])
    for t in range(tensors):
        done = totals[t].astype(jnp.bfloat16) if full_tiles else totals[t]
        for i, r in enumerate(o_refs):
            piece = done[i * part : (i + 1) * part].reshape(sources, rows, HEAD_PAIR)
            r[:, t, item, :, lanes] = piece.astype(jnp.bfloat16)


def attention_kernel(*refs):
    x_refs, o_refs = refs[: len(refs) // 2], refs[len(refs) // 2 :]
    items, feats = x_refs[0].shape[2], x_refs[0].shape[4]
    for item in range(items):
        for pair in range(feats // HEAD_PAIR):
            attend(x_refs, o_refs, item, pl.ds(pair * HEAD_PAIR, HEAD_PAIR))


def attention(pieces):
    spec = pl.BlockSpec(memory_space=pltpu.VMEM)
    return pl.pallas_call(
        attention_kernel,
        in_specs=[spec] * len(pieces),
        out_specs=[spec] * len(pieces),
        out_shape=[jax.ShapeDtypeStruct(p.shape, p.dtype) for p in pieces],
    )(*pieces)


def shift(piece, far, by):
    if by % FACTOR == 0:
        return piece
    place = lambda x, z: x * FACTOR + z
    pairs = []
    for x in range(FACTOR):
        for z in range(FACTOR):
            to = place(x, (z + by) % FACTOR) if far else place((x + by) % FACTOR, z)
            pairs.append((place(x, z), to))
    return lax.ppermute(piece, "lat", pairs)


def on_device(*inputs):
    batch, rows, cols, feats = inputs[0].shape
    tensors = len(inputs)
    lon = lax.axis_size("lon")
    lat = lax.axis_size("lat")
    lon_items = batch * rows // lon
    lat_items = batch * cols // lat
    part = lat_items // CHUNKS
    me = lax.axis_index("lat")
    near, far = me // FACTOR, me % FACTOR
    swap_lon = lambda t: lax.all_to_all(t, "lon", split_axis=0, concat_axis=0, tiled=True)
    pick = lambda t, i: lax.dynamic_index_in_dim(t, i % FACTOR, 0, keepdims=False)

    lon_got = swap_lon(jnp.stack([t.reshape(lon, lon_items, cols, feats) for t in inputs], axis=1))
    send = jnp.stack([t.transpose(0, 2, 1, 3).reshape(lat, lat_items, rows, feats) for t in inputs], axis=1)
    send = send.reshape((FACTOR, FACTOR) + send.shape[1:])
    turned = jnp.stack([shift(pick(send, near + m), False, m) for m in range(FACTOR)], axis=1)
    home = []
    for c in range(CHUNKS):
        mine = turned[:, :, :, c * part : (c + 1) * part]
        got = [shift(pick(mine, far + k), True, k) for k in range(FACTOR)]
        done = attention(got)
        home.append([shift(done[k], True, -k) for k in range(FACTOR)])
    (lon_done,) = attention([lon_got])
    lon_back = swap_lon(lon_done)
    joined = [jnp.concatenate([h[k] for h in home], axis=2) for k in range(FACTOR)]
    back = [shift(jnp.stack([j[m] for j in joined], axis=0), False, -m) for m in range(FACTOR)]
    lat_back = jnp.roll(jnp.roll(jnp.stack(back, axis=0), near, axis=0), far, axis=1)
    lat_back = lat_back.reshape((lat,) + lat_back.shape[2:])
    results = []
    for i in range(tensors):
        a = lon_back[:, i].reshape(batch, rows, cols, feats)
        b = lat_back[:, i].reshape(batch, cols, rows, feats).transpose(0, 2, 1, 3)
        results.append((a.astype(jnp.float32) + b.astype(jnp.float32)).astype(jnp.bfloat16))
    return tuple(results)


def solution(mesh):
    spec = P(None, "lat", "lon", None)
    return jax.shard_map(on_device, mesh=mesh, in_specs=(spec,) * 4, out_specs=(spec,) * 4, check_vma=False)
```

```python
import jax
import jax.numpy as jnp
from jax import lax
from jax.experimental import pallas as pl
from jax.experimental.pallas import tpu as pltpu
from jax.sharding import PartitionSpec as P


HEAD_DIM = 64
HEAD_PAIR = 2 * HEAD_DIM
FACTOR = 4


def attend(x_refs, o_refs, item, lanes):
    sources, tensors, _, rows, _ = x_refs[0].shape
    part = sources * rows
    length = part * len(x_refs)
    scale = HEAD_DIM ** (-0.5)
    full_tiles = rows % 8 == 0

    def whole(t):
        if full_tiles:
            return jnp.concatenate([r[:, t, item, :, lanes].reshape(part, HEAD_PAIR) for r in x_refs], axis=0)
        parts = [r[:, t, item, :, lanes].astype(jnp.float32).reshape(part, HEAD_PAIR) for r in x_refs]
        return jnp.concatenate(parts, axis=0).astype(jnp.bfloat16)

    q, k, v, g = (whole(t) for t in range(tensors))
    lane = lax.broadcasted_iota(jnp.int32, (length, HEAD_PAIR), 1)
    nt, nn, tn = ((((1,), (1,)), ((), ())), (((1,), (0,)), ((), ())), (((0,), (0,)), ((), ())))
    dot = lambda a, b, dims: lax.dot_general(a, b, dims, preferred_element_type=jnp.float32)
    totals = None
    for h in range(HEAD_PAIR // HEAD_DIM):
        mine = lane // HEAD_DIM == h
        qh, kh, vh, gh = (jnp.where(mine, t, jnp.zeros_like(t)) for t in (q, k, v, g))
        scores = dot(qh, k, nt) * scale
        exps = jnp.exp(scores - jnp.max(scores, axis=-1, keepdims=True))
        probs = exps * (1.0 / jnp.sum(exps, axis=-1, keepdims=True))
        rounded = probs.astype(jnp.bfloat16)
        grad_probs = dot(gh, v, nt)
        row_delta = jnp.sum(probs * grad_probs, axis=-1, keepdims=True)
        grad_scores = (probs * (grad_probs - row_delta)).astype(jnp.bfloat16)
        parts = (dot(rounded, vh, nn), dot(grad_scores, kh, nn), dot(grad_scores, qh, tn), dot(rounded, gh, tn))
        totals = parts if totals is None else tuple(a + b for a, b in zip(totals, parts))
    totals = (totals[0], totals[1] * scale, totals[2] * scale, totals[3])
    for t in range(tensors):
        done = totals[t].astype(jnp.bfloat16) if full_tiles else totals[t]
        done = done.reshape(len(x_refs), sources, rows, HEAD_PAIR)
        for i, r in enumerate(o_refs):
            piece = done[:, i] if len(o_refs) > 1 else done[0]
            r[:, t, item, :, lanes] = piece.astype(jnp.bfloat16)


def attention_kernel(*refs):
    x_refs, o_refs = refs[: len(refs) // 2], refs[len(refs) // 2 :]
    items, feats = x_refs[0].shape[2], x_refs[0].shape[4]
    for item in range(items):
        for pair in range(feats // HEAD_PAIR):
            attend(x_refs, o_refs, item, pl.ds(pair * HEAD_PAIR, HEAD_PAIR))


def attention(pieces):
    spec = pl.BlockSpec(memory_space=pltpu.VMEM)
    return pl.pallas_call(
        attention_kernel,
        in_specs=[spec] * len(pieces),
        out_specs=[spec] * len(pieces),
        out_shape=[jax.ShapeDtypeStruct(p.shape, p.dtype) for p in pieces],
    )(*pieces)


def shift(piece, far, by):
    if by % FACTOR == 0:
        return piece
    place = lambda x, z: x * FACTOR + z
    pairs = []
    for x in range(FACTOR):
        for z in range(FACTOR):
            to = place(x, (z + by) % FACTOR) if far else place((x + by) % FACTOR, z)
            pairs.append((place(x, z), to))
    return lax.ppermute(piece, "lat", pairs)


def on_device(*inputs):
    batch, rows, cols, feats = inputs[0].shape
    tensors = len(inputs)
    lon = lax.axis_size("lon")
    lat = lax.axis_size("lat")
    lon_items = batch * rows // lon
    lat_items = batch * cols // lat
    me = lax.axis_index("lat")
    near, far = me // FACTOR, me % FACTOR
    swap_lon = lambda t: lax.all_to_all(t, "lon", split_axis=0, concat_axis=0, tiled=True)
    pick = lambda t, i: lax.dynamic_index_in_dim(t, i % FACTOR, 0, keepdims=False)

    lon_got = swap_lon(jnp.stack([t.reshape(lon, lon_items, cols, feats) for t in inputs], axis=1))
    send = jnp.stack([t.transpose(0, 2, 1, 3).reshape(lat, lat_items, rows, feats) for t in inputs], axis=1)
    send = send.reshape((FACTOR, FACTOR) + send.shape[1:])
    turned = jnp.stack([shift(pick(send, near + m), False, m) for m in range(FACTOR)], axis=1)
    lat_got = [shift(pick(turned, far + k), True, k) for k in range(FACTOR)]
    (lon_done,) = attention([lon_got])
    lon_back = swap_lon(lon_done)
    lat_done = attention(lat_got)
    back = [shift(lat_done[m], False, -m) for m in range(FACTOR)]
    home = [shift(jnp.stack([b[k] for b in back], axis=0), True, -k) for k in range(FACTOR)]
    lat_back = jnp.stack([pick(jnp.stack(home, axis=0), z - far) for z in range(FACTOR)], axis=1)
    lat_back = jnp.stack([pick(lat_back, x - near) for x in range(FACTOR)], axis=0)
    lat_back = lat_back.reshape((lat,) + lat_back.shape[2:])
    results = []
    for i in range(tensors):
        a = lon_back[:, i].reshape(batch, rows, cols, feats)
        b = lat_back[:, i].reshape(batch, cols, rows, feats).transpose(0, 2, 1, 3)
        results.append((a.astype(jnp.float32) + b.astype(jnp.float32)).astype(jnp.bfloat16))
    return tuple(results)


def solution(mesh):
    spec = P(None, "lat", "lon", None)
    return jax.shard_map(on_device, mesh=mesh, in_specs=(spec,) * 4, out_specs=(spec,) * 4, check_vma=False)
```

```python
import jax
import jax.numpy as jnp
from jax import lax
from jax.experimental import pallas as pl
from jax.experimental.pallas import tpu as pltpu
from jax.sharding import PartitionSpec as P


HEAD_DIM = 64
HEAD_PAIR = 2 * HEAD_DIM
FACTOR = 4


def attend(x_refs, o_refs, item, lanes):
    sources, tensors, _, rows, _ = x_refs[0].shape
    part = sources * rows
    length = part * len(x_refs)
    scale = HEAD_DIM ** (-0.5)
    full_tiles = rows % 8 == 0

    def whole(t):
        if full_tiles:
            return jnp.concatenate([r[:, t, item, :, lanes].reshape(part, HEAD_PAIR) for r in x_refs], axis=0)
        parts = [r[:, t, item, :, lanes].astype(jnp.float32).reshape(part, HEAD_PAIR) for r in x_refs]
        return jnp.concatenate(parts, axis=0).astype(jnp.bfloat16)

    q, k, v, g = (whole(t) for t in range(tensors))
    lane = lax.broadcasted_iota(jnp.int32, (length, HEAD_PAIR), 1)
    nt, nn, tn = ((((1,), (1,)), ((), ())), (((1,), (0,)), ((), ())), (((0,), (0,)), ((), ())))
    dot = lambda a, b, dims: lax.dot_general(a, b, dims, preferred_element_type=jnp.float32)
    totals = None
    for h in range(HEAD_PAIR // HEAD_DIM):
        mine = lane // HEAD_DIM == h
        qh, kh, vh, gh = (jnp.where(mine, t, jnp.zeros_like(t)) for t in (q, k, v, g))
        scores = dot(qh, k, nt) * scale
        exps = jnp.exp(scores - jnp.max(scores, axis=-1, keepdims=True))
        probs = exps * (1.0 / jnp.sum(exps, axis=-1, keepdims=True))
        rounded = probs.astype(jnp.bfloat16)
        grad_probs = dot(gh, v, nt)
        row_delta = jnp.sum(probs * grad_probs, axis=-1, keepdims=True)
        grad_scores = (probs * (grad_probs - row_delta)).astype(jnp.bfloat16)
        parts = (dot(rounded, vh, nn), dot(grad_scores, kh, nn), dot(grad_scores, qh, tn), dot(rounded, gh, tn))
        totals = parts if totals is None else tuple(a + b for a, b in zip(totals, parts))
    totals = (totals[0], totals[1] * scale, totals[2] * scale, totals[3])
    for t in range(tensors):
        done = totals[t].astype(jnp.bfloat16) if full_tiles else totals[t]
        done = done.reshape(len(x_refs), sources, rows, HEAD_PAIR)
        for i, r in enumerate(o_refs):
            piece = done[:, i] if len(o_refs) > 1 else done[0]
            r[:, t, item, :, lanes] = piece.astype(jnp.bfloat16)


def attention_kernel(*refs):
    x_refs, o_refs = refs[: len(refs) // 2], refs[len(refs) // 2 :]
    items, feats = x_refs[0].shape[2], x_refs[0].shape[4]
    for item in range(items):
        for pair in range(feats // HEAD_PAIR):
            attend(x_refs, o_refs, item, pl.ds(pair * HEAD_PAIR, HEAD_PAIR))


def attention(pieces, near_core):
    spec = pl.BlockSpec(memory_space=pltpu.VMEM)
    if near_core:
        pieces = [pltpu.with_memory_space_constraint(p, pltpu.VMEM) for p in pieces]
    return pl.pallas_call(
        attention_kernel,
        in_specs=[spec] * len(pieces),
        out_specs=[spec] * len(pieces),
        out_shape=[pltpu.VMEM(p.shape, p.dtype) if near_core else jax.ShapeDtypeStruct(p.shape, p.dtype) for p in pieces],
    )(*pieces)


def shift(piece, far, by):
    if by % FACTOR == 0:
        return piece
    place = lambda x, z: x * FACTOR + z
    pairs = []
    for x in range(FACTOR):
        for z in range(FACTOR):
            to = place(x, (z + by) % FACTOR) if far else place((x + by) % FACTOR, z)
            pairs.append((place(x, z), to))
    return lax.ppermute(piece, "lat", pairs)


def on_device(*inputs):
    batch, rows, cols, feats = inputs[0].shape
    tensors = len(inputs)
    lon = lax.axis_size("lon")
    lat = lax.axis_size("lat")
    lon_items = batch * rows // lon
    lat_items = batch * cols // lat
    me = lax.axis_index("lat")
    near, far = me // FACTOR, me % FACTOR
    swap_lon = lambda t: lax.all_to_all(t, "lon", split_axis=0, concat_axis=0, tiled=True)
    pick = lambda t, i: lax.dynamic_index_in_dim(t, i % FACTOR, 0, keepdims=False)

    lon_got = swap_lon(jnp.stack([t.reshape(lon, lon_items, cols, feats) for t in inputs], axis=1))
    send = jnp.stack([t.transpose(0, 2, 1, 3).reshape(lat, lat_items, rows, feats) for t in inputs], axis=1)
    send = send.reshape((FACTOR, FACTOR) + send.shape[1:])
    turned = jnp.stack([shift(pick(send, near + m), False, m) for m in range(FACTOR)], axis=1)
    lat_got = [shift(pick(turned, far + k), True, k) for k in range(FACTOR)]
    (lon_done,) = attention([lon_got], False)
    lon_back = swap_lon(lon_done)
    lat_done = attention(lat_got, True)
    back = [shift(lat_done[m], False, -m) for m in range(FACTOR)]
    home = [shift(jnp.stack([b[k] for b in back], axis=0), True, -k) for k in range(FACTOR)]
    lat_back = jnp.stack([pick(jnp.stack(home, axis=0), z - far) for z in range(FACTOR)], axis=1)
    lat_back = jnp.stack([pick(lat_back, x - near) for x in range(FACTOR)], axis=0)
    lat_back = lat_back.reshape((lat,) + lat_back.shape[2:])
    results = []
    for i in range(tensors):
        a = lon_back[:, i].reshape(batch, rows, cols, feats)
        b = lat_back[:, i].reshape(batch, cols, rows, feats).transpose(0, 2, 1, 3)
        results.append((a.astype(jnp.float32) + b.astype(jnp.float32)).astype(jnp.bfloat16))
    return tuple(results)


def solution(mesh):
    spec = P(None, "lat", "lon", None)
    return jax.shard_map(on_device, mesh=mesh, in_specs=(spec,) * 4, out_specs=(spec,) * 4, check_vma=False)
```

```python
import jax
import jax.numpy as jnp
from jax import lax
from jax.experimental import pallas as pl
from jax.experimental.pallas import tpu as pltpu
from jax.sharding import PartitionSpec as P


HEAD_DIM = 64
HEAD_PAIR = 2 * HEAD_DIM
FACTOR = 4


def attend(x_refs, o_refs, item, lanes):
    sources, tensors, _, rows, _ = x_refs[0].shape
    part = sources * rows
    length = part * len(x_refs)
    scale = HEAD_DIM ** (-0.5)
    full_tiles = rows % 8 == 0

    def whole(t):
        if full_tiles:
            return jnp.concatenate([r[:, t, item, :, lanes].reshape(part, HEAD_PAIR) for r in x_refs], axis=0)
        parts = [r[:, t, item, :, lanes].astype(jnp.float32).reshape(part, HEAD_PAIR) for r in x_refs]
        return jnp.concatenate(parts, axis=0).astype(jnp.bfloat16)

    q, k, v, g = (whole(t) for t in range(tensors))
    lane = lax.broadcasted_iota(jnp.int32, (length, HEAD_PAIR), 1)
    nt, nn, tn = ((((1,), (1,)), ((), ())), (((1,), (0,)), ((), ())), (((0,), (0,)), ((), ())))
    dot = lambda a, b, dims: lax.dot_general(a, b, dims, preferred_element_type=jnp.float32)
    totals = None
    for h in range(HEAD_PAIR // HEAD_DIM):
        mine = lane // HEAD_DIM == h
        qh, kh, vh, gh = (jnp.where(mine, t, jnp.zeros_like(t)) for t in (q, k, v, g))
        scores = dot(qh, k, nt) * scale
        exps = jnp.exp(scores - jnp.max(scores, axis=-1, keepdims=True))
        probs = exps * (1.0 / jnp.sum(exps, axis=-1, keepdims=True))
        rounded = probs.astype(jnp.bfloat16)
        grad_probs = dot(gh, v, nt)
        row_delta = jnp.sum(probs * grad_probs, axis=-1, keepdims=True)
        grad_scores = (probs * (grad_probs - row_delta)).astype(jnp.bfloat16)
        parts = (dot(rounded, vh, nn), dot(grad_scores, kh, nn), dot(grad_scores, qh, tn), dot(rounded, gh, tn))
        totals = parts if totals is None else tuple(a + b for a, b in zip(totals, parts))
    totals = (totals[0], totals[1] * scale, totals[2] * scale, totals[3])
    for t in range(tensors):
        done = totals[t].astype(jnp.bfloat16) if full_tiles else totals[t]
        done = done.reshape(len(x_refs), sources, rows, HEAD_PAIR)
        for i, r in enumerate(o_refs):
            piece = done[:, i] if len(o_refs) > 1 else done[0]
            r[:, t, item, :, lanes] = piece.astype(jnp.bfloat16)


def attention_kernel(*refs):
    x_refs, o_refs = refs[: len(refs) // 2], refs[len(refs) // 2 :]
    items, feats = x_refs[0].shape[2], x_refs[0].shape[4]
    for item in range(items):
        for pair in range(feats // HEAD_PAIR):
            attend(x_refs, o_refs, item, pl.ds(pair * HEAD_PAIR, HEAD_PAIR))


def attention(pieces, near_core):
    spec = pl.BlockSpec(memory_space=pltpu.VMEM)
    if near_core:
        pieces = [pltpu.with_memory_space_constraint(p, pltpu.VMEM) for p in pieces]
    return pl.pallas_call(
        attention_kernel,
        in_specs=[spec] * len(pieces),
        out_specs=[spec] * len(pieces),
        out_shape=[pltpu.VMEM(p.shape, p.dtype) if near_core else jax.ShapeDtypeStruct(p.shape, p.dtype) for p in pieces],
    )(*pieces)


def finish_kernel(places, lat_ref, lon_ref, *o_refs):
    items, _, _ = lat_ref.shape[3:]
    cols = lon_ref.shape[3]
    first = pl.program_id(0) * (cols // items)
    for t, o_ref in enumerate(o_refs):
        lat_cols = []
        for c in range(cols):
            to = first + c // items
            near = (to // FACTOR - places[0]) % FACTOR
            far = (to % FACTOR - places[1]) % FACTOR
            lat_cols.append(lat_ref[far, near, t, c % items].astype(jnp.float32))
        lat_part = jnp.stack(lat_cols, axis=1)
        o_ref[0] = (lon_ref[:, t, 0].astype(jnp.float32) + lat_part).astype(jnp.bfloat16)


def finish(places, lat_back, lon_back, shape):
    batch, rows, cols, feats = shape
    tensors = lon_back.shape[1]
    lat_back = pltpu.with_memory_space_constraint(lat_back, pltpu.VMEM)
    return pl.pallas_call(
        finish_kernel,
        grid=(batch,),
        in_specs=[
            pl.BlockSpec(memory_space=pltpu.SMEM),
            pl.BlockSpec(memory_space=pltpu.VMEM),
            pl.BlockSpec((rows, tensors, 1, cols, feats), lambda b: (b, 0, 0, 0, 0)),
        ],
        out_specs=[pl.BlockSpec((1, rows, cols, feats), lambda b: (b, 0, 0, 0))] * tensors,
        out_shape=[jax.ShapeDtypeStruct(shape, jnp.bfloat16)] * tensors,
    )(places, lat_back, lon_back)


def shift(piece, far, by):
    if by % FACTOR == 0:
        return piece
    place = lambda x, z: x * FACTOR + z
    pairs = []
    for x in range(FACTOR):
        for z in range(FACTOR):
            to = place(x, (z + by) % FACTOR) if far else place((x + by) % FACTOR, z)
            pairs.append((place(x, z), to))
    return lax.ppermute(piece, "lat", pairs)


def on_device(*inputs):
    batch, rows, cols, feats = inputs[0].shape
    tensors = len(inputs)
    lon = lax.axis_size("lon")
    lat = lax.axis_size("lat")
    lon_items = batch * rows // lon
    lat_items = batch * cols // lat
    me = lax.axis_index("lat")
    near, far = me // FACTOR, me % FACTOR
    swap_lon = lambda t: lax.all_to_all(t, "lon", split_axis=0, concat_axis=0, tiled=True)
    pick = lambda t, i: lax.dynamic_index_in_dim(t, i % FACTOR, 0, keepdims=False)

    lon_got = swap_lon(jnp.stack([t.reshape(lon, lon_items, cols, feats) for t in inputs], axis=1))
    send = jnp.stack([t.transpose(0, 2, 1, 3).reshape(lat, lat_items, rows, feats) for t in inputs], axis=1)
    send = send.reshape((FACTOR, FACTOR) + send.shape[1:])
    turned = jnp.stack([shift(pick(send, near + m), False, m) for m in range(FACTOR)], axis=1)
    lat_got = [shift(pick(turned, far + k), True, k) for k in range(FACTOR)]
    (lon_done,) = attention([lon_got], False)
    lon_back = swap_lon(lon_done)
    lat_done = attention(lat_got, True)
    back = [shift(lat_done[m], False, -m) for m in range(FACTOR)]
    home = [shift(jnp.stack([b[k] for b in back], axis=0), True, -k) for k in range(FACTOR)]
    places = jnp.stack([near, far]).astype(jnp.int32)
    rows_back = lon_back.transpose(0, 2, 1, 3, 4).reshape(batch * rows, tensors, 1, cols, feats)
    return finish(places, jnp.stack(home, axis=0), rows_back, inputs[0].shape)


def solution(mesh):
    spec = P(None, "lat", "lon", None)
    return jax.shard_map(on_device, mesh=mesh, in_specs=(spec,) * 4, out_specs=(spec,) * 4, check_vma=False)
```
